256 devices in a mesh: tm: 64 (over x_hi, z, y), space: 4 (over x_lo, core).
Axes of the slice: x: 4 (x_hi: 2, x_lo: 2; x = x_hi * 2 + x_lo), y: 4, z: 8, core: 2. Of those that a mesh axis runs over, the one named last changes fastest.
Arguments:
- volume: float32 [64, 16, 256, 256], P('tm', 'space'), may hold values from -6 to 6
- prior_image: float32 [64, 16, 256, 256], P('tm', 'space'), may hold values from -6 to 6
- dual_pairs: float32 [64, 4, 16, 256, 256], P('tm', None, 'space'), may hold values from -0.3 to 0.3
- pair_cycle: int32 [64, 4], P('tm'), may hold values from -2 to 2, as said below
- pair_offset: int32 [64, 4], P('tm'), may hold values from -3 to 3
Outputs:
- volume_next: float32 [64, 16, 256, 256], P('tm', 'space')
- dual_next: float32 [64, 4, 16, 256, 256], P('tm', None, 'space')
The draws below stay inside these ranges and needn't reach their ends.
Inputs may be any that keep to these rules, and one draw needn't show every extreme that they name: `pair_cycle`: each frame has at least one filled slot; filled slots come first, name distinct cycle offsets, and always name a partner frame inside 0 .. 63.
All inputs are finite; a program needn't handle non-finite values.
Results may differ from the reference program's by a relative error of at most 0.0003.
Values sent between devices are 32-bit elements; how exact they have to be, the bound alone decides.
A program may use at most 64 MiB of HBM per device.

```python
import jax
import jax.numpy as jnp
from jax import lax

NY = 256
NX = 256
PAIRS = 4
CYCLES = 8
FRAMES = 64
Z = 16


def draw_pair_cycle(key, part):
    stride = FRAMES // CYCLES
    frames = jnp.arange(FRAMES, dtype=jnp.int32)[:, None]
    hop_table = jnp.array([-2, -1, 1, 2], jnp.int32)[None, :]
    target_frame = frames + hop_table * stride
    validity = ((target_frame >= 0) & (target_frame < FRAMES)).astype(jnp.int32)
    order_key = jax.random.fold_in(key, 11)
    count_key = jax.random.fold_in(key, 23)
    row_keys = jax.random.split(order_key, FRAMES)
    priority = jax.vmap(lambda subkey: jax.random.permutation(subkey, 4))(row_keys).astype(jnp.int32)
    scores = validity * 8 + priority
    ranking = jnp.argsort(-scores, axis=1)
    live_count = jax.random.randint(count_key, (FRAMES, 1), 1, 5).astype(jnp.int32)
    live_count = jnp.minimum(live_count, jnp.sum(validity, axis=1, keepdims=True))
    picked = jnp.take_along_axis(hop_table * jnp.ones_like(validity), ranking, axis=1)
    slot_index = jnp.arange(4, dtype=jnp.int32)[None, :]
    return jnp.where(slot_index < live_count, picked, 0).astype(jnp.int32)


def with_ends(result, key, low, high):
    longest = result.shape.index(max(result.shape))
    spots = []
    for shift in (0, 1):
        where = [jax.random.randint(jax.random.fold_in(key, axis), (), 0, length) for axis, length in enumerate(result.shape)]
        where[longest] = (where[longest] + shift) % result.shape[longest]
        spots.append(tuple(where))
    return result.at[spots[0]].set(low).at[spots[1]].set(high)


def levels(stream_key, shape, pieces, low, high):
    gain = 1.0
    for dim, blocks in pieces:
        steps = jax.random.uniform(jax.random.fold_in(jax.random.fold_in(stream_key, 6), dim), (blocks,), jnp.float32, low / len(pieces), high / len(pieces))
        gain = gain * jnp.repeat(jnp.exp(steps), shape[dim] // blocks).reshape((-1,) + (1,) * (len(shape) - 1 - dim))
    return gain


def centred(own_key, shape, spread, bound, pieces=(), held_as=jnp.bfloat16):
    drawn = spread * jax.random.normal(own_key, shape, jnp.float32)
    if pieces:
        drawn = drawn * levels(own_key, shape, pieces, -0.22, 0.18)
    return jnp.clip(drawn, -bound, bound).astype(held_as)


def setup_inputs(seed: int = 0) -> dict:
    keys = jax.random.split(jax.random.key(seed), 6)
    volume = centred(keys[0], (FRAMES, Z, NY, NX), 1.0, 6.0, ((0, 64), (1, 4)), jnp.float32)
    prior_image = centred(keys[1], (FRAMES, Z, NY, NX), 1.0, 6.0, ((0, 64), (1, 4)), jnp.float32)
    dual_pairs = jnp.clip(jax.random.uniform(keys[2], (FRAMES, PAIRS, Z, NY, NX), jnp.float32, -0.3, 0.3) * levels(keys[2], (FRAMES, PAIRS, Z, NY, NX), ((0, 64), (2, 4)), -0.4, 0.0), -0.3, 0.3)
    pair_cycle = draw_pair_cycle(jax.random.fold_in(keys[5], 71), 0)
    pair_offset = with_ends(jax.random.randint(keys[4], (FRAMES, PAIRS), -3, 4), jax.random.fold_in(keys[4], 1), -3, 3).astype(jnp.int32)
    return {"volume": volume, "prior_image": prior_image, "dual_pairs": dual_pairs, "pair_cycle": pair_cycle, "pair_offset": pair_offset}


dual_step = 0.5
primal_step = 0.25
dual_bound = 0.3
fidelity = 1.0


def shift_rows(field, offset):
    lead = [(0, 0)] * (field.ndim - 2)
    padded = jnp.pad(field, lead + [(3, 3), (0, 0)])
    start = (3 - offset).astype(jnp.int32)
    return lax.dynamic_slice_in_dim(padded, start, field.shape[-2], field.ndim - 2)


def unshift_rows(field, offset):
    lead = [(0, 0)] * (field.ndim - 2)
    padded = jnp.pad(field, lead + [(3, 3), (0, 0)])
    start = (3 + offset).astype(jnp.int32)
    return lax.dynamic_slice_in_dim(padded, start, field.shape[-2], field.ndim - 2)


def box_mean(field):
    zsum = field[..., :-2, :, :] + field[..., 1:-1, :, :] + field[..., 2:, :, :]
    lead = [(0, 0)] * (zsum.ndim - 2)
    padded = jnp.pad(zsum, lead + [(1, 1), (0, 0)])
    ysum = padded[..., :-2, :] + padded[..., 1:-1, :] + padded[..., 2:, :]
    padded = jnp.pad(ysum, [(0, 0)] * (ysum.ndim - 1) + [(1, 1)])
    return (padded[..., :-2] + padded[..., 1:-1] + padded[..., 2:]) / 27.0


def reference(volume, prior_image, dual_pairs, pair_cycle, pair_offset):
    stride = FRAMES // CYCLES

    def frame_step(frame):
        current = volume[frame]
        fresh_list = []
        outgoing_list = []
        local_sum = jnp.zeros_like(current)
        for slot in range(PAIRS):
            cycle = pair_cycle[frame, slot]
            active = cycle != 0
            target = jnp.clip(frame + cycle * stride, 0, FRAMES - 1).astype(jnp.int32)
            partner = jnp.where(active, volume[target], jnp.zeros_like(current))
            shifted = shift_rows(partner, pair_offset[frame, slot])
            contrast = shifted - current
            squares = jnp.pad(contrast * contrast, ((1, 1), (0, 0), (0, 0)))
            weight_root = jnp.exp(-box_mean(squares) / 4.0)
            fresh = jnp.clip(dual_pairs[frame, slot] + dual_step * weight_root * contrast, -dual_bound, dual_bound)
            fresh = jnp.where(active, fresh, jnp.zeros_like(fresh))
            flux = weight_root * fresh
            local_sum = local_sum + flux
            fresh_list.append(fresh)
            outgoing_list.append(unshift_rows(flux, pair_offset[frame, slot]))
        return jnp.stack(fresh_list), local_sum, jnp.stack(outgoing_list)

    frames = jnp.arange(FRAMES, dtype=jnp.int32)
    dual_next, local_sums, outgoing = lax.map(frame_step, frames)

    def gather_step(frame):
        incoming = jnp.zeros(volume.shape[1:], jnp.float32)
        for hop_count in (-2, -1, 1, 2):
            source = frame - hop_count * stride
            inside = (source >= 0) & (source < FRAMES)
            source_clip = jnp.clip(source, 0, FRAMES - 1).astype(jnp.int32)
            for slot in range(PAIRS):
                match = inside & (pair_cycle[source_clip, slot] == hop_count)
                incoming = incoming + jnp.where(match, outgoing[source_clip, slot], jnp.zeros_like(incoming))
        return incoming

    incoming = lax.map(gather_step, frames)
    volume_next = (volume - primal_step * (incoming - local_sums) + primal_step * fidelity * prior_image) / (1.0 + primal_step * fidelity)
    return volume_next, dual_next
```

```python
import functools

import jax
import jax.numpy as jnp
from jax import lax
from jax.experimental import pallas as pl
from jax.experimental.pallas import tpu as pltpu
from jax.sharding import PartitionSpec as P

MESH = pl.DeviceIdType.MESH

NZ, NY = 4, 256
LANES, HALVES = 128, 2
PAD = 8
ROWS = NY + 2 * PAD
CHUNK = 64

NAMES = []
for stem, slices in (
    ("P", (0, 1, 2, 3)),
    ("M", (0, 1, 2, 3)),
    ("PR", (0, 1)),
    ("MR", (2, 3)),
    ("XW", (0, 1, 2, 3)),
    ("XO", (0, 1, 2, 3)),
    ("XV", (0, 1, 2, 3)),
    ("HL", (0, 1, 2, 3, 4)),
    ("HH", (0, 1, 2, 3, 4)),
    ("FX", (0, 1, 2, 3)),
    ("XD", (0, 1, 2, 3)),
    ("FO", (0, 1, 2, 3)),
    ("PD", (2, 3)),
    ("MD", (0, 1)),
    ("PF", (0, 1)),
    ("MF", (2, 3)),
    ("PS", (0, 1)),
    ("MS", (2, 3)),
):
    NAMES += [(stem, j) for j in slices]
SEM = {name: i for i, name in enumerate(NAMES)}


def when(pred, fn):
    if pred is None:
        fn()
    else:
        pl.when(pred)(fn)


def kernel(
    cyc, off, vol, pri, dua, vn_out, dn_out,
    OWN, R1, R3, R2, X2, W, V, T, Z, FL, DU, FR, F1P, F1M, F2, FX, XF1, XF2,
    RP, RM, SP, SM, INM, INP, LS, PRI, VN, ss, rs, ls,
):
    tm = lax.axis_index("tm")
    s = lax.axis_index("space")
    h = tm // 32
    z = (tm // 4) % 8
    y = tm % 4
    pos = z // 2
    c = 4 * h + pos
    plus = (h * 32 + ((z + 2) % 8) * 4 + y, s)
    minus = (h * 32 + ((z + 6) % 8) * 4 + y, s)
    across = ((1 - h) * 32 + z * 4 + y, s)
    below = (tm, lax.max(s - 1, 0))
    above = (tm, lax.min(s + 1, 3))
    has_below = s > 0
    has_above = s < 3
    first, last = c == 0, c == 7
    is3, is4 = c == 3, c == 4
    inner = jnp.logical_and(c > 1, c < 6)
    outer = jnp.logical_not(inner)

    def copy(name, src, dst, target):
        i = SEM[name]
        return pltpu.make_async_remote_copy(
            src_ref=src, dst_ref=dst, send_sem=ss.at[i], recv_sem=rs.at[i],
            device_id=target, device_id_type=MESH,
        )

    sent = []

    def send(name, src, dst, target, pred=None):
        when(pred, lambda: copy(name, src, dst, target).start())
        sent.append((name, target, pred))

    def arrive(name, dst, pred=None):
        when(pred, lambda: copy(name, dst, dst, across).wait_recv())

    def img(ref, k):
        return ref.at[k, :, pl.ds(PAD, NY), :]

    class Split:
        def __init__(self, make):
            self.copies = [make(b, pl.ds(b * LANES, LANES)) for b in range(HALVES)]

        def start(self):
            for one in self.copies:
                one.start()

        def wait(self):
            for one in self.copies:
                one.wait()

    own_in = [
        Split(lambda b, cols, j=j: pltpu.make_async_copy(vol.at[0, j, :, cols], OWN.at[1 + j, b], ls.at[j, b]))
        for j in range(NZ)
    ]
    for j in (0, 3, 1, 2):
        own_in[j].start()

    barrier = pltpu.get_barrier_semaphore()
    for target, pred in ((plus, None), (minus, None), (across, None), (below, has_below), (above, has_above)):
        when(pred, lambda target=target: pl.semaphore_signal(barrier, inc=1, device_id=target, device_id_type=MESH))
    dual_in = Split(lambda b, cols: pltpu.make_async_copy(dua.at[0, :, :, :, cols], DU.at[:, :, b], ls.at[4, b]))
    prior_in = Split(lambda b, cols: pltpu.make_async_copy(pri.at[0, :, :, cols], PRI.at[:, b], ls.at[5, b]))
    pl.semaphore_wait(barrier, 3 + has_below.astype(jnp.int32) + has_above.astype(jnp.int32))

    not_p3 = pos < 3
    not_p0 = pos > 0
    not_first, not_last = jnp.logical_not(first), jnp.logical_not(last)

    def send_own(sign, j):
        src = OWN.at[1 + j]
        if sign > 0:
            name, target, inside, edge, spare, into = ("P", j), plus, not_p3, pos == 3, last, img(R3, 1 + j)
            direct = j >= 2
        else:
            name, target, inside, edge, spare, into = ("M", j), minus, not_p0, pos == 0, first, img(R1, 1 + j)
            direct = j < 2
        send(name, src, into, target, inside)
        if direct:
            arrive(("XV", j), V.at[j], spare)
            send(name, V.at[j], into, target, spare)
        else:
            send(name, src, W.at[j], target, edge)

    def send_across():
        for j in (3, 2):
            send(("XV", j), OWN.at[1 + j], V.at[j], across, c == 3)
        for j in (0, 1):
            send(("XV", j), OWN.at[1 + j], V.at[j], across, c == 4)

    def halo(i, ref, k, src=None, pred=None):
        own = ref is OWN
        at = (lambda k: ref.at[k]) if own else (lambda k: img(ref, k))
        both = lambda a: a if pred is None else jnp.logical_and(a, pred)
        if k == 1:
            send(("HL", i), at(1), at(5), below, both(has_below))
        else:
            send(("HH", i), at(4), at(0), above, both(has_above))

    def halo_arrive(i, ref, pred=None):
        own = ref is OWN
        at = (lambda k: ref.at[k]) if own else (lambda k: img(ref, k))
        both = lambda a: a if pred is None else jnp.logical_and(a, pred)
        arrive(("HL", i), at(5), both(has_above))
        arrive(("HH", i), at(0), both(has_below))

    own_in[0].wait()
    send_own(1, 0)
    own_in[3].wait()
    send_own(-1, 3)
    own_in[1].wait()
    send_own(1, 1)
    own_in[2].wait()
    send_own(-1, 2)
    send_across()
    halo(0, OWN, 1)
    halo(0, OWN, 4)
    dual_in.start()
    prior_in.start()

    zeros = jnp.zeros((6, HALVES, PAD, LANES), jnp.float32)
    for ref in (R1, R3, R2, X2):
        ref[:, :, pl.ds(0, PAD), :] = zeros
        ref[:, :, pl.ds(PAD + NY, PAD), :] = zeros
    for ref in (Z, FL):
        ref[:, pl.ds(0, PAD), :] = zeros[0]
        ref[:, pl.ds(PAD + NY, PAD), :] = zeros[0]

    @pl.when(s == 0)
    def _():
        T[0] = jnp.zeros((HALVES, NY, LANES), jnp.float32)

    @pl.when(s == 3)
    def _():
        T[5] = jnp.zeros((HALVES, NY, LANES), jnp.float32)

    def got_plus(j):
        if j < 2:
            arrive(("P", j), img(R3, 1 + j), not_p0)
            arrive(("P", j), W.at[j], pos == 0)
            send(("PR", j), img(R3, 1 + j), img(R2, 1 + j), plus, not_p0)
            send(("PR", j), W.at[j], img(R2, 1 + j), plus, pos == 0)
            send(("XW", j), W.at[j], img(R3, 1 + j), across, first)
            if j == 0:
                halo(2, R3, 1, pred=not_p0)
        else:
            arrive(("P", j), img(R3, 1 + j), not_first)
            if j == 3:
                halo(2, R3, 4, pred=not_first)

    def got_minus(j):
        if j >= 2:
            arrive(("M", j), img(R1, 1 + j), not_p3)
            arrive(("M", j), W.at[j], pos == 3)
            send(("MR", j), img(R1, 1 + j), img(R2, 1 + j), minus, not_p3)
            send(("MR", j), W.at[j], img(R2, 1 + j), minus, pos == 3)
            send(("XW", j), W.at[j], img(R1, 1 + j), across, last)
            if j == 3:
                halo(1, R1, 4, pred=not_p3)
        else:
            arrive(("M", j), img(R1, 1 + j), not_last)
            if j == 0:
                halo(1, R1, 1, pred=not_last)

    up = (0, 1, 3, 2)
    down = (3, 2, 0, 1)

    def own(rank):
        send_own(1, up[rank])
        send_own(-1, down[rank])

    def got(rank):
        got_plus(up[rank])
        got_minus(down[rank])

    def got_opposite(name, j):
        arrive((name, j), img(R2, 1 + j))
        send(("XO", j), img(R2, 1 + j), img(X2, 1 + j), across, outer)
        if j in (0, 3):
            halo(3, R2, 1 + j)

    lane = lax.broadcasted_iota(jnp.int32, (CHUNK, LANES), 1)
    left, right = lane == 0, lane == LANES - 1
    k_lo = 1 - has_below.astype(jnp.int32)
    k_hi = 5 + has_above.astype(jnp.int32)
    chunks = NY // CHUNK

    def pair(p, direction, ref, out, fresh_sum, order, emit):
        slot = jnp.int32(0)
        shift = jnp.int32(0)
        active = jnp.int32(0)
        for k in range(4):
            hit = cyc[0, k] == direction
            slot = slot + jnp.where(hit, k, 0)
            shift = shift + jnp.where(hit, off[0, k], 0)
            active = active + jnp.where(hit, 1, 0)
        live = active > 0

        def contrast(k, b, r):
            return ref[k, b, pl.ds(PAD - shift + r, CHUNK), :] - OWN[k, b, pl.ds(r, CHUNK), :]

        def squares(k, carry):
            for q in range(chunks):
                r = q * CHUNK
                x0, x1 = contrast(k, 0, r), contrast(k, 1, r)
                x0, x1 = x0 * x0, x1 * x1
                l0, l1 = pltpu.roll(x0, 1, 1), pltpu.roll(x1, 1, 1)
                r0, r1 = pltpu.roll(x0, LANES - 1, 1), pltpu.roll(x1, LANES - 1, 1)
                T[k, 0, pl.ds(r, CHUNK), :] = x0 + jnp.where(left, 0.0, l0) + jnp.where(right, r1, r0)
                T[k, 1, pl.ds(r, CHUNK), :] = x1 + jnp.where(left, l0, l1) + jnp.where(right, 0.0, r1)
            return carry

        lax.fori_loop(k_lo, k_hi, squares, 0)

        def update(j):
            for b in range(HALVES):
                for q in range(chunks):
                    rows = pl.ds(q * CHUNK, CHUNK)
                    Z[b, pl.ds(PAD + q * CHUNK, CHUNK), :] = T[j, b, rows, :] + T[j + 1, b, rows, :] + T[j + 2, b, rows, :]
                for q in range(chunks):
                    r = q * CHUNK
                    rows = pl.ds(r, CHUNK)
                    total = (
                        Z[b, pl.ds(PAD - 1 + r, CHUNK), :]
                        + Z[b, pl.ds(PAD + r, CHUNK), :]
                        + Z[b, pl.ds(PAD + 1 + r, CHUNK), :]
                    )
                    w = jnp.exp(total * (-1.0 / 108.0))
                    fresh = jnp.clip(DU[slot, j, b, rows, :] + 0.5 * w * contrast(j + 1, b, r), -0.3, 0.3)
                    fresh = jnp.where(live, fresh, 0.0)
                    FR[p, j, b, rows, :] = fresh
                    flux = w * fresh
                    if fresh_sum:
                        LS[j, b, rows, :] = flux
                    else:
                        LS[j, b, rows, :] = LS[j, b, rows, :] + flux
                    FL[b, pl.ds(PAD + r, CHUNK), :] = flux
                for q in range(chunks):
                    r = q * CHUNK
                    out[j, b, pl.ds(r, CHUNK), :] = FL[b, pl.ds(PAD + shift + r, CHUNK), :]

        for n, j in enumerate(order):
            update(j)
            if n > 0:
                emit(order[n - 1])
        emit(order[-1])

    forward = pos < 2
    def opposite(rank):
        got_opposite("PR", rank)
        got_opposite("MR", 3 - rank)

    def send_far(pred, j):
        if j < 2:
            send(("PF", j), F2.at[j], RP.at[j], plus, pred)
        else:
            send(("MF", j), F2.at[j], RM.at[j - 2], minus, pred)

    def pair_far():
        halo_arrive(3, R2)
        pair(2, jnp.where(forward, 2, -2), R2, F2, True, (0, 3, 1, 2), functools.partial(send_far, inner))

    def pair_across():
        for j in (0, 3, 1, 2):
            arrive(("XO", j), img(X2, 1 + j), inner)
            if j in (0, 3):
                halo(4, X2, 1 + j, pred=inner)
        halo_arrive(4, X2, inner)

        def emit(j):
            send(("FO", j), FX.at[j], XF2.at[j], across, inner)

        @pl.when(inner)
        def _():
            pair(3, jnp.where(forward, -2, 2), X2, FX, False, (0, 3, 1, 2), emit)

    def got_across():
        for j in (3, 2):
            arrive(("XW", j), img(R1, 1 + j), c == 3)
        halo(1, R1, 4, pred=c == 3)
        for j in (0, 1):
            arrive(("XW", j), img(R3, 1 + j), c == 4)
        halo(2, R3, 1, pred=c == 4)

    def pair_next():
        halo_arrive(1, R1, not_last)

        def emit(j):
            if j < 2:
                send(("FX", j), F1P.at[j], XF1.at[j], across, is3)
            else:
                send(("PD", j), F1P.at[j], INM.at[j], plus, not_last)

        @pl.when(not_last)
        def _():
            pair(0, 1, R1, F1P, False, (2, 3, 0, 1), emit)

    def pair_before():
        halo_arrive(2, R3, not_first)

        def emit(j):
            if j < 2:
                send(("MD", j), F1M.at[j], INP.at[j], minus, not_first)
            else:
                send(("FX", j), F1M.at[j], XF1.at[j], across, is4)

        @pl.when(not_first)
        def _():
            pair(1, -1, R3, F1M, False, (1, 0, 3, 2), emit)

    def far_outer():
        for j in (0, 3, 1, 2):
            arrive(("FO", j), XF2.at[j], outer)

            @pl.when(outer)
            def _():
                F2[j] = F2[j] + XF2[j]

            if j == 0 or j == 1:
                send(("PF", j), F2.at[j], RP.at[j], plus, outer)
            else:
                send(("MF", j), F2.at[j], RM.at[j - 2], minus, outer)

    halo_arrive(0, OWN)
    dual_in.wait()
    got(0)
    own(2)
    got(1)
    own(3)
    opposite(0)
    opposite(1)
    pair_far()
    got(2)
    pair_across()
    got(3)
    got_across()
    pair_next()
    pair_before()
    far_outer()

    for j in (0, 1):
        arrive(("FX", j), XF1.at[j], last)
    for j in (3, 2):
        arrive(("FX", j), XF1.at[j], first)

    def pass_on():
        for j in (2, 3):
            arrive(("PD", j), INM.at[j], first)
            send(("XD", j), INM.at[j], INM.at[j], across, first)
        for j in (1, 0):
            arrive(("MD", j), INP.at[j], last)
            send(("XD", j), INP.at[j], INP.at[j], across, last)

    def slot_out(k):
        cycle = cyc[0, k]
        hop = jnp.where(cycle > 0, 0, 1)
        far = jnp.where((cycle > 0) == forward, 2, 3)
        p = jnp.where(jnp.logical_or(cycle == 1, cycle == -1), hop, far)

        def put(j, carry):
            DU[k, j] = jnp.where(cycle != 0, FR[p, j], 0.0)
            return carry

        lax.fori_loop(0, NZ, put, 0)

    for k in range(4):
        slot_out(k)
    dual_out = Split(lambda b, cols: pltpu.make_async_copy(DU.at[:, :, b], dn_out.at[0, :, :, :, cols], ls.at[6, b]))
    dual_out.start()
    prior_in.wait()

    def start_volume(j, carry):
        VN[j] = OWN[1 + j] + 0.25 * LS[j] + 0.25 * PRI[j]
        return carry

    lax.fori_loop(0, NZ, start_volume, 0)

    def second(name, onward, rel, sums, base, spare, j, i, target, none, swap, dst):
        arrive((name, j), rel.at[i])

        @pl.when(none)
        def _():
            sums[i] = rel[i]

        @pl.when(swap)
        def _():
            sums[i] = rel[i] + spare[j]

        @pl.when(jnp.logical_not(jnp.logical_or(none, swap)))
        def _():
            sums[i] = rel[i] + base[j]

        send((onward, j), sums.at[i], dst.at[j], target)

    second("PF", "PS", RP, SP, F1P, XF1, 0, 0, plus, c == 3, last, INM)
    second("MF", "MS", RM, SM, F1M, XF1, 3, 1, minus, c == 4, first, INP)
    pass_on()
    second("PF", "PS", RP, SP, F1P, XF1, 1, 1, plus, c == 3, last, INM)
    second("MF", "MS", RM, SM, F1M, XF1, 2, 0, minus, c == 4, first, INP)

    def take(ref, j):
        VN[j] = VN[j] - 0.25 * ref[j]

    for j in (2, 3):
        arrive(("PD", j), INM.at[j], jnp.logical_and(c != 4, not_first))
        arrive(("XD", j), INM.at[j], c == 4)
        pl.when(not_first)(functools.partial(take, INM, j))
    for j in (1, 0):
        arrive(("MD", j), INP.at[j], jnp.logical_and(c != 3, not_last))
        arrive(("XD", j), INP.at[j], c == 3)
        pl.when(not_last)(functools.partial(take, INP, j))

    outs = []
    for name, ref, j in (("PS", INM, 0), ("MS", INP, 3), ("PS", INM, 1), ("MS", INP, 2)):
        arrive((name, j), ref.at[j])
        VN[j] = (VN[j] - 0.25 * ref[j]) / 1.25
        outs.append(
            Split(lambda b, cols, j=j: pltpu.make_async_copy(VN.at[j, b], vn_out.at[0, j, :, cols], ls.at[j, b]))
        )
        outs[-1].start()

    for name, target, pred in sent:
        when(pred, lambda: copy(name, OWN.at[0], OWN.at[0], target).wait_send())
    for out in outs:
        out.wait()
    dual_out.wait()


def shards(volume, prior_image, dual_pairs, pair_cycle, pair_offset):
    image = pltpu.VMEM((NZ + 2, HALVES, ROWS, LANES), jnp.float32)
    block = pltpu.VMEM((NZ, HALVES, NY, LANES), jnp.float32)
    half = pltpu.VMEM((2, HALVES, NY, LANES), jnp.float32)
    plane = pltpu.VMEM((HALVES, ROWS, LANES), jnp.float32)
    stack = pltpu.VMEM((NZ + 2, HALVES, NY, LANES), jnp.float32)
    slots = pltpu.VMEM((4, NZ, HALVES, NY, LANES), jnp.float32)
    smem = pl.BlockSpec(memory_space=pltpu.SMEM)
    anyspace = pl.BlockSpec(memory_space=pl.ANY)
    return pl.pallas_call(
        kernel,
        out_shape=(
            pltpu.VMEM(volume.shape, jnp.float32),
            pltpu.VMEM(dual_pairs.shape, jnp.float32),
        ),
        in_specs=[smem, smem, anyspace, anyspace, anyspace],
        out_specs=(anyspace, anyspace),
        scratch_shapes=[
            stack, image, image, image, image, block, block,
            stack, plane, plane, slots, slots,
            block, block, block, block, block, block,
            half, half, half, half, block, block,
            block, block, block,
            pltpu.SemaphoreType.DMA((len(NAMES),)),
            pltpu.SemaphoreType.DMA((len(NAMES),)),
            pltpu.SemaphoreType.DMA((7, HALVES)),
        ],
        compiler_params=pltpu.CompilerParams(collective_id=0, vmem_limit_bytes=61_790_000, has_side_effects=True),
    )(pair_cycle, pair_offset, volume, prior_image, dual_pairs)


def solution(mesh):
    return jax.shard_map(
        shards,
        mesh=mesh,
        in_specs=(
            P("tm", "space", None, None),
            P("tm", "space", None, None),
            P("tm", None, "space", None, None),
            P("tm", None),
            P("tm", None),
        ),
        out_specs=(P("tm", "space", None, None), P("tm", None, "space", None, None)),
        check_vma=False,
    )
```

```python
import functools

import jax
import jax.numpy as jnp
from jax import lax
from jax.experimental import pallas as pl
from jax.experimental.pallas import tpu as pltpu
from jax.sharding import PartitionSpec as P

MESH = pl.DeviceIdType.MESH

NZ, NY = 4, 256
LANES, HALVES = 128, 2
PAD = 8
ROWS = NY + 2 * PAD
CHUNK = 64

NAMES = []
for stem, slices in (
    ("P", (0, 1, 2, 3)),
    ("M", (0, 1, 2, 3)),
    ("PR", (0, 1)),
    ("MR", (2, 3)),
    ("XW", (0, 1, 2, 3)),
    ("XO", (0, 1, 2, 3)),
    ("XV", (0, 1, 2, 3)),
    ("HL", (0, 1, 2, 3, 4)),
    ("HH", (0, 1, 2, 3, 4)),
    ("FX", (0, 1, 2, 3)),
    ("XD", (0, 1, 2, 3)),
    ("FO", (0, 1, 2, 3)),
    ("PD", (2, 3)),
    ("MD", (0, 1)),
    ("PF", (0, 1)),
    ("MF", (2, 3)),
    ("PS", (0, 1)),
    ("MS", (2, 3)),
):
    NAMES += [(stem, j) for j in slices]
SEM = {name: i for i, name in enumerate(NAMES)}


def when(pred, fn):
    if pred is None:
        fn()
    else:
        pl.when(pred)(fn)


class Image:
    def __init__(self, main, late=None, late_k=None):
        self.main, self.late, self.late_k = main, late, late_k

    def block(self, k):
        if self.late is not None and k == self.late_k:
            return self.late.at[:, pl.ds(PAD, NY), :]
        return self.main.at[k, :, pl.ds(PAD, NY), :]

    def load(self, k, b, start):
        if self.late is not None and k == self.late_k:
            return self.late[b, pl.ds(start, CHUNK), :]
        return self.main[k, b, pl.ds(start, CHUNK), :]


def kernel(
    cyc, off, vol, pri, dua, vn_out, dn_out,
    OWN, R1, R3, R2, X2, R1L, R3L, W, V, T, T1, T3, Z, FL, DU, FR, F1P, F1M, F2, FX, XF1, XF2,
    RP, RM, SP, SM, INM, INP, LS, PRI, VN, ss, rs, ls,
):
    R1, R3, R2, X2 = Image(R1, R1L, 2), Image(R3, R3L, 3), Image(R2), Image(X2)
    tm = lax.axis_index("tm")
    s = lax.axis_index("space")
    h = tm // 32
    z = (tm // 4) % 8
    y = tm % 4
    pos = z // 2
    c = 4 * h + pos
    plus = (h * 32 + ((z + 2) % 8) * 4 + y, s)
    minus = (h * 32 + ((z + 6) % 8) * 4 + y, s)
    across = ((1 - h) * 32 + z * 4 + y, s)
    below = (tm, lax.max(s - 1, 0))
    above = (tm, lax.min(s + 1, 3))
    has_below = s > 0
    has_above = s < 3
    first, last = c == 0, c == 7
    is3, is4 = c == 3, c == 4
    inner = jnp.logical_and(c > 1, c < 6)
    outer = jnp.logical_not(inner)

    def copy(name, src, dst, target):
        i = SEM[name]
        return pltpu.make_async_remote_copy(
            src_ref=src, dst_ref=dst, send_sem=ss.at[i], recv_sem=rs.at[i],
            device_id=target, device_id_type=MESH,
        )

    sent = []

    def send(name, src, dst, target, pred=None):
        when(pred, lambda: copy(name, src, dst, target).start())
        sent.append((name, target, pred))

    def arrive(name, dst, pred=None):
        when(pred, lambda: copy(name, dst, dst, across).wait_recv())

    def img(ref, k):
        return ref.block(k)

    class Split:
        def __init__(self, make):
            self.copies = [make(b, pl.ds(b * LANES, LANES)) for b in range(HALVES)]

        def start(self):
            for one in self.copies:
                one.start()

        def wait(self):
            for one in self.copies:
                one.wait()

    own_in = [
        Split(lambda b, cols, j=j: pltpu.make_async_copy(vol.at[0, j, :, cols], OWN.at[1 + j, b], ls.at[j, b]))
        for j in range(NZ)
    ]
    for j in (0, 3, 1, 2):
        own_in[j].start()

    barrier = pltpu.get_barrier_semaphore()
    for target, pred in ((plus, None), (minus, None), (across, None), (below, has_below), (above, has_above)):
        when(pred, lambda target=target: pl.semaphore_signal(barrier, inc=1, device_id=target, device_id_type=MESH))
    dual_in = Split(lambda b, cols: pltpu.make_async_copy(dua.at[0, :, :, :, cols], DU.at[:, :, b], ls.at[4, b]))
    prior_in = Split(lambda b, cols: pltpu.make_async_copy(pri.at[0, :, :, cols], PRI.at[:, b], ls.at[5, b]))
    pl.semaphore_wait(barrier, 3 + has_below.astype(jnp.int32) + has_above.astype(jnp.int32))

    not_p3 = pos < 3
    not_p0 = pos > 0
    not_first, not_last = jnp.logical_not(first), jnp.logical_not(last)

    def send_own(sign, j):
        src = OWN.at[1 + j]
        if sign > 0:
            name, target, inside, edge, spare, into = ("P", j), plus, not_p3, pos == 3, last, img(R3, 1 + j)
            direct = j >= 2
        else:
            name, target, inside, edge, spare, into = ("M", j), minus, not_p0, pos == 0, first, img(R1, 1 + j)
            direct = j < 2
        send(name, src, into, target, inside)
        if direct:
            arrive(("XV", j), V.at[j], spare)
            send(name, V.at[j], into, target, spare)
        else:
            send(name, src, W.at[j], target, edge)

    def send_across():
        for j in (3, 2):
            send(("XV", j), OWN.at[1 + j], V.at[j], across, c == 3)
        for j in (0, 1):
            send(("XV", j), OWN.at[1 + j], V.at[j], across, c == 4)

    def halo(i, ref, k, src=None, pred=None):
        own = ref is OWN
        at = (lambda k: ref.at[k]) if own else (lambda k: img(ref, k))
        both = lambda a: a if pred is None else jnp.logical_and(a, pred)
        if k == 1:
            send(("HL", i), at(1), at(5), below, both(has_below))
        else:
            send(("HH", i), at(4), at(0), above, both(has_above))

    def halo_arrive(i, ref, pred=None):
        own = ref is OWN
        at = (lambda k: ref.at[k]) if own else (lambda k: img(ref, k))
        both = lambda a: a if pred is None else jnp.logical_and(a, pred)
        arrive(("HL", i), at(5), both(has_above))
        arrive(("HH", i), at(0), both(has_below))

    own_in[0].wait()
    send_own(1, 0)
    own_in[3].wait()
    send_own(-1, 3)
    own_in[1].wait()
    send_own(1, 1)
    own_in[2].wait()
    send_own(-1, 2)
    send_across()
    halo(0, OWN, 1)
    halo(0, OWN, 4)
    dual_in.start()
    prior_in.start()

    zeros = jnp.zeros((6, HALVES, PAD, LANES), jnp.float32)
    for ref in (R1.main, R3.main, R2.main, X2.main):
        ref[:, :, pl.ds(0, PAD), :] = zeros
        ref[:, :, pl.ds(PAD + NY, PAD), :] = zeros
    for ref in (Z, FL, R1L, R3L):
        ref[:, pl.ds(0, PAD), :] = zeros[0]
        ref[:, pl.ds(PAD + NY, PAD), :] = zeros[0]

    @pl.when(s == 0)
    def _():
        for sums in (T, T1, T3):
            sums[0] = jnp.zeros((HALVES, NY, LANES), jnp.float32)

    @pl.when(s == 3)
    def _():
        for sums in (T, T1, T3):
            sums[5] = jnp.zeros((HALVES, NY, LANES), jnp.float32)

    def got_plus(j):
        if j < 2:
            arrive(("P", j), img(R3, 1 + j), not_p0)
            arrive(("P", j), W.at[j], pos == 0)
            send(("PR", j), img(R3, 1 + j), img(R2, 1 + j), plus, not_p0)
            send(("PR", j), W.at[j], img(R2, 1 + j), plus, pos == 0)
            send(("XW", j), W.at[j], img(R3, 1 + j), across, first)
            if j == 0:
                halo(2, R3, 1, pred=not_p0)
        else:
            arrive(("P", j), img(R3, 1 + j), not_first)
            if j == 3:
                halo(2, R3, 4, pred=not_first)

    def got_minus(j):
        if j >= 2:
            arrive(("M", j), img(R1, 1 + j), not_p3)
            arrive(("M", j), W.at[j], pos == 3)
            send(("MR", j), img(R1, 1 + j), img(R2, 1 + j), minus, not_p3)
            send(("MR", j), W.at[j], img(R2, 1 + j), minus, pos == 3)
            send(("XW", j), W.at[j], img(R1, 1 + j), across, last)
            if j == 3:
                halo(1, R1, 4, pred=not_p3)
        else:
            arrive(("M", j), img(R1, 1 + j), not_last)
            if j == 0:
                halo(1, R1, 1, pred=not_last)

    up = (0, 1, 3, 2)
    down = (3, 2, 0, 1)

    def own(rank):
        send_own(1, up[rank])
        send_own(-1, down[rank])

    def got(rank):
        got_plus(up[rank])
        got_minus(down[rank])

    def got_opposite(name, j):
        arrive((name, j), img(R2, 1 + j))
        send(("XO", j), img(R2, 1 + j), img(X2, 1 + j), across, outer)
        if j in (0, 3):
            halo(3, R2, 1 + j)

    lane = lax.broadcasted_iota(jnp.int32, (CHUNK, LANES), 1)
    left, right = lane == 0, lane == LANES - 1
    k_lo = 1 - has_below.astype(jnp.int32)
    k_hi = 5 + has_above.astype(jnp.int32)
    chunks = NY // CHUNK

    def pair(p, direction, ref, out, fresh_sum, T):
        slot = jnp.int32(0)
        shift = jnp.int32(0)
        active = jnp.int32(0)
        for k in range(4):
            hit = cyc[0, k] == direction
            slot = slot + jnp.where(hit, k, 0)
            shift = shift + jnp.where(hit, off[0, k], 0)
            active = active + jnp.where(hit, 1, 0)
        live = active > 0

        def contrast(k, b, r):
            return ref.load(k, b, PAD - shift + r) - OWN[k, b, pl.ds(r, CHUNK), :]

        def squares(k):
            for q in range(chunks):
                r = q * CHUNK
                x0, x1 = contrast(k, 0, r), contrast(k, 1, r)
                x0, x1 = x0 * x0, x1 * x1
                l0, l1 = pltpu.roll(x0, 1, 1), pltpu.roll(x1, 1, 1)
                r0, r1 = pltpu.roll(x0, LANES - 1, 1), pltpu.roll(x1, LANES - 1, 1)
                T[k, 0, pl.ds(r, CHUNK), :] = x0 + jnp.where(left, 0.0, l0) + jnp.where(right, r1, r0)
                T[k, 1, pl.ds(r, CHUNK), :] = x1 + jnp.where(left, l0, l1) + jnp.where(right, 0.0, r1)

        def update(j):
            for b in range(HALVES):
                for q in range(chunks):
                    rows = pl.ds(q * CHUNK, CHUNK)
                    Z[b, pl.ds(PAD + q * CHUNK, CHUNK), :] = T[j, b, rows, :] + T[j + 1, b, rows, :] + T[j + 2, b, rows, :]
                for q in range(chunks):
                    r = q * CHUNK
                    rows = pl.ds(r, CHUNK)
                    total = (
                        Z[b, pl.ds(PAD - 1 + r, CHUNK), :]
                        + Z[b, pl.ds(PAD + r, CHUNK), :]
                        + Z[b, pl.ds(PAD + 1 + r, CHUNK), :]
                    )
                    w = jnp.exp(total * (-1.0 / 108.0))
                    fresh = jnp.clip(DU[slot, j, b, rows, :] + 0.5 * w * contrast(j + 1, b, r), -0.3, 0.3)
                    fresh = jnp.where(live, fresh, 0.0)
                    FR[p, j, b, rows, :] = fresh
                    flux = w * fresh
                    if fresh_sum:
                        LS[j, b, rows, :] = flux
                    else:
                        LS[j, b, rows, :] = LS[j, b, rows, :] + flux
                    FL[b, pl.ds(PAD + r, CHUNK), :] = flux
                for q in range(chunks):
                    r = q * CHUNK
                    out[j, b, pl.ds(r, CHUNK), :] = FL[b, pl.ds(PAD + shift + r, CHUNK), :]

        return squares, update

    def all_squares(squares):
        def one(k, carry):
            squares(k)
            return carry

        lax.fori_loop(k_lo, k_hi, one, 0)

    def updates(update, order, emit):
        for n, j in enumerate(order):
            update(j)
            if n > 0:
                emit(order[n - 1])
        emit(order[-1])

    forward = pos < 2
    def opposite(rank):
        got_opposite("PR", rank)
        got_opposite("MR", 3 - rank)

    def send_far(pred, j):
        if j < 2:
            send(("PF", j), F2.at[j], RP.at[j], plus, pred)
        else:
            send(("MF", j), F2.at[j], RM.at[j - 2], minus, pred)

    def pair_far():
        halo_arrive(3, R2)
        squares, update = pair(2, jnp.where(forward, 2, -2), R2, F2, True, T)
        all_squares(squares)
        updates(update, (0, 3, 1, 2), functools.partial(send_far, inner))

    def pair_across():
        for j in (0, 3, 1, 2):
            arrive(("XO", j), img(X2, 1 + j), inner)
            if j in (0, 3):
                halo(4, X2, 1 + j, pred=inner)
        halo_arrive(4, X2, inner)

        def emit(j):
            send(("FO", j), FX.at[j], XF2.at[j], across, inner)

        @pl.when(inner)
        def _():
            squares, update = pair(3, jnp.where(forward, -2, 2), X2, FX, False, T)
            all_squares(squares)
            updates(update, (0, 3, 1, 2), emit)

    def got_across():
        for j in (3, 2):
            arrive(("XW", j), img(R1, 1 + j), c == 3)
        halo(1, R1, 4, pred=c == 3)
        for j in (0, 1):
            arrive(("XW", j), img(R3, 1 + j), c == 4)
        halo(2, R3, 1, pred=c == 4)

    next_squares, next_update = pair(0, 1, R1, F1P, False, T1)
    before_squares, before_update = pair(1, -1, R3, F1M, False, T3)

    def next_emit(j):
        if j < 2:
            send(("FX", j), F1P.at[j], XF1.at[j], across, is3)
        else:
            send(("PD", j), F1P.at[j], INM.at[j], plus, not_last)

    def before_emit(j):
        if j < 2:
            send(("MD", j), F1M.at[j], INP.at[j], minus, not_first)
        else:
            send(("FX", j), F1M.at[j], XF1.at[j], across, is4)

    def early():
        halo_arrive(1, R1, not_last)

        @pl.when(not_last)
        def _():
            pl.when(has_above)(functools.partial(next_squares, 5))
            next_squares(4)
            next_squares(3)
            next_update(3)

        halo_arrive(2, R3, not_first)

        @pl.when(not_first)
        def _():
            pl.when(has_below)(functools.partial(before_squares, 0))
            before_squares(1)
            before_squares(2)
            before_update(0)

        next_emit(3)
        before_emit(0)

        @pl.when(not_last)
        def _():
            pl.when(has_below)(functools.partial(next_squares, 0))
            next_squares(1)

        @pl.when(not_first)
        def _():
            pl.when(has_above)(functools.partial(before_squares, 5))
            before_squares(4)

    def late():
        @pl.when(not_last)
        def _():
            next_squares(2)
            next_update(2)

        @pl.when(not_first)
        def _():
            before_squares(3)
            before_update(1)

        next_emit(2)
        before_emit(1)

        @pl.when(not_last)
        def _():
            updates(next_update, (0, 1), next_emit)

        @pl.when(not_first)
        def _():
            updates(before_update, (3, 2), before_emit)

    def far_outer():
        for j in (0, 3, 1, 2):
            arrive(("FO", j), XF2.at[j], outer)

            @pl.when(outer)
            def _():
                F2[j] = F2[j] + XF2[j]

            if j == 0 or j == 1:
                send(("PF", j), F2.at[j], RP.at[j], plus, outer)
            else:
                send(("MF", j), F2.at[j], RM.at[j - 2], minus, outer)

    halo_arrive(0, OWN)
    dual_in.wait()
    got(0)
    own(2)
    got(1)
    own(3)
    opposite(0)
    opposite(1)
    pair_far()
    got(2)
    pair_across()
    got_across()
    early()
    got(3)
    late()
    far_outer()

    for j in (0, 1):
        arrive(("FX", j), XF1.at[j], last)
    for j in (3, 2):
        arrive(("FX", j), XF1.at[j], first)

    def pass_on():
        for j in (3, 2):
            arrive(("PD", j), INM.at[j], first)
            send(("XD", j), INM.at[j], INM.at[j], across, first)
        for j in (0, 1):
            arrive(("MD", j), INP.at[j], last)
            send(("XD", j), INP.at[j], INP.at[j], across, last)

    def slot_out(k):
        cycle = cyc[0, k]
        hop = jnp.where(cycle > 0, 0, 1)
        far = jnp.where((cycle > 0) == forward, 2, 3)
        p = jnp.where(jnp.logical_or(cycle == 1, cycle == -1), hop, far)

        def put(j, carry):
            DU[k, j] = jnp.where(cycle != 0, FR[p, j], 0.0)
            return carry

        lax.fori_loop(0, NZ, put, 0)

    for k in range(4):
        slot_out(k)
    dual_out = Split(lambda b, cols: pltpu.make_async_copy(DU.at[:, :, b], dn_out.at[0, :, :, :, cols], ls.at[6, b]))
    dual_out.start()
    prior_in.wait()

    def start_volume(j, carry):
        VN[j] = OWN[1 + j] + 0.25 * LS[j] + 0.25 * PRI[j]
        return carry

    lax.fori_loop(0, NZ, start_volume, 0)

    def second(name, onward, rel, sums, base, spare, j, i, target, none, swap, dst):
        arrive((name, j), rel.at[i])

        @pl.when(none)
        def _():
            sums[i] = rel[i]

        @pl.when(swap)
        def _():
            sums[i] = rel[i] + spare[j]

        @pl.when(jnp.logical_not(jnp.logical_or(none, swap)))
        def _():
            sums[i] = rel[i] + base[j]

        send((onward, j), sums.at[i], dst.at[j], target)

    second("PF", "PS", RP, SP, F1P, XF1, 0, 0, plus, c == 3, last, INM)
    second("MF", "MS", RM, SM, F1M, XF1, 3, 1, minus, c == 4, first, INP)
    pass_on()
    second("PF", "PS", RP, SP, F1P, XF1, 1, 1, plus, c == 3, last, INM)
    second("MF", "MS", RM, SM, F1M, XF1, 2, 0, minus, c == 4, first, INP)

    def take(ref, j):
        VN[j] = VN[j] - 0.25 * ref[j]

    for j in (2, 3):
        arrive(("PD", j), INM.at[j], jnp.logical_and(c != 4, not_first))
        arrive(("XD", j), INM.at[j], c == 4)
        pl.when(not_first)(functools.partial(take, INM, j))
    for j in (1, 0):
        arrive(("MD", j), INP.at[j], jnp.logical_and(c != 3, not_last))
        arrive(("XD", j), INP.at[j], c == 3)
        pl.when(not_last)(functools.partial(take, INP, j))

    outs = []
    for name, ref, j in (("PS", INM, 0), ("MS", INP, 3), ("PS", INM, 1), ("MS", INP, 2)):
        arrive((name, j), ref.at[j])
        VN[j] = (VN[j] - 0.25 * ref[j]) / 1.25
        outs.append(
            Split(lambda b, cols, j=j: pltpu.make_async_copy(VN.at[j, b], vn_out.at[0, j, :, cols], ls.at[j, b]))
        )
        outs[-1].start()

    for name, target, pred in sent:
        when(pred, lambda: copy(name, OWN.at[0], OWN.at[0], target).wait_send())
    for out in outs:
        out.wait()
    dual_out.wait()


def shards(volume, prior_image, dual_pairs, pair_cycle, pair_offset):
    image = pltpu.VMEM((NZ + 2, HALVES, ROWS, LANES), jnp.float32)
    block = pltpu.VMEM((NZ, HALVES, NY, LANES), jnp.float32)
    half = pltpu.VMEM((2, HALVES, NY, LANES), jnp.float32)
    plane = pltpu.VMEM((HALVES, ROWS, LANES), jnp.float32)
    stack = pltpu.VMEM((NZ + 2, HALVES, NY, LANES), jnp.float32)
    slots = pltpu.VMEM((4, NZ, HALVES, NY, LANES), jnp.float32)
    smem = pl.BlockSpec(memory_space=pltpu.SMEM)
    anyspace = pl.BlockSpec(memory_space=pl.ANY)
    return pl.pallas_call(
        kernel,
        out_shape=(
            pltpu.VMEM(volume.shape, jnp.float32),
            pltpu.VMEM(dual_pairs.shape, jnp.float32),
        ),
        in_specs=[smem, smem, anyspace, anyspace, anyspace],
        out_specs=(anyspace, anyspace),
        scratch_shapes=[
            stack, image, image, image, image, plane, plane, block, block,
            stack, stack, stack, plane, plane, slots, slots,
            block, block, block, block, block, block,
            half, half, half, half, block, block,
            block, block, block,
            pltpu.SemaphoreType.DMA((len(NAMES),)),
            pltpu.SemaphoreType.DMA((len(NAMES),)),
            pltpu.SemaphoreType.DMA((7, HALVES)),
        ],
        compiler_params=pltpu.CompilerParams(collective_id=0, vmem_limit_bytes=61_790_000, has_side_effects=True),
    )(pair_cycle, pair_offset, volume, prior_image, dual_pairs)


def solution(mesh):
    return jax.shard_map(
        shards,
        mesh=mesh,
        in_specs=(
            P("tm", "space", None, None),
            P("tm", "space", None, None),
            P("tm", None, "space", None, None),
            P("tm", None),
            P("tm", None),
        ),
        out_specs=(P("tm", "space", None, None), P("tm", None, "space", None, None)),
        check_vma=False,
    )
```

```python
import functools

import jax
import jax.numpy as jnp
from jax import lax
from jax.experimental import pallas as pl
from jax.experimental.pallas import tpu as pltpu
from jax.sharding import PartitionSpec as P

MESH = pl.DeviceIdType.MESH

NZ, NY = 4, 256
LANES, HALVES = 128, 2
PAD = 8
ROWS = NY + 2 * PAD
CHUNK = 64

NAMES = []
for stem, slices in (
    ("P", (0, 1, 2, 3)),
    ("M", (0, 1, 2, 3)),
    ("PR", (0, 1)),
    ("MR", (2, 3)),
    ("XW", (0, 1, 2, 3)),
    ("XO", (0, 1, 2, 3)),
    ("XV", (0, 1, 2, 3)),
    ("HL", (0, 1, 2, 3, 4)),
    ("HH", (0, 1, 2, 3, 4)),
    ("FX", (0, 1, 2, 3)),
    ("XD", (0, 1, 2, 3)),
    ("FO", (0, 1, 2, 3)),
    ("PD", (2, 3)),
    ("MD", (0, 1)),
    ("PF", (0, 1)),
    ("MF", (2, 3)),
    ("PS", (0, 1)),
    ("MS", (2, 3)),
):
    NAMES += [(stem, j) for j in slices]
SEM = {name: i for i, name in enumerate(NAMES)}


def when(pred, fn):
    if pred is None:
        fn()
    else:
        pl.when(pred)(fn)


class Image:
    def __init__(self, main, late=None, late_k=None):
        self.main, self.late, self.late_k = main, late, late_k

    def block(self, k):
        if self.late is not None and k == self.late_k:
            return self.late.at[:, pl.ds(PAD, NY), :]
        return self.main.at[k, :, pl.ds(PAD, NY), :]

    def load(self, k, b, start):
        if self.late is not None and k == self.late_k:
            return self.late[b, pl.ds(start, CHUNK), :]
        return self.main[k, b, pl.ds(start, CHUNK), :]


def kernel(
    cyc, off, vol, pri, dua, vn_out, dn_out,
    OWN, R1, R3, R2, X2, R1L, R3L, W, V, T, T1, T3, Z, FL, DU, FR, F1P, F1M, F2, FX, XF1, XF2,
    RP, RM, SP, SM, INM, INP, LS, PRI, VN, ss, rs, ls,
):
    R1, R3, R2, X2 = Image(R1, R1L, 2), Image(R3, R3L, 3), Image(R2), Image(X2)
    tm = lax.axis_index("tm")
    s = lax.axis_index("space")
    h = tm // 32
    z = (tm // 4) % 8
    y = tm % 4
    pos = z // 2
    c = 4 * h + pos
    plus = (h * 32 + ((z + 2) % 8) * 4 + y, s)
    minus = (h * 32 + ((z + 6) % 8) * 4 + y, s)
    across = ((1 - h) * 32 + z * 4 + y, s)
    below = (tm, lax.max(s - 1, 0))
    above = (tm, lax.min(s + 1, 3))
    has_below = s > 0
    has_above = s < 3
    first, last = c == 0, c == 7
    is3, is4 = c == 3, c == 4
    inner = jnp.logical_and(c > 1, c < 6)
    outer = jnp.logical_not(inner)

    def copy(name, src, dst, target):
        i = SEM[name]
        return pltpu.make_async_remote_copy(
            src_ref=src, dst_ref=dst, send_sem=ss.at[i], recv_sem=rs.at[i],
            device_id=target, device_id_type=MESH,
        )

    sent = []

    def send(name, src, dst, target, pred=None):
        when(pred, lambda: copy(name, src, dst, target).start())
        sent.append((name, target, pred))

    def arrive(name, dst, pred=None):
        when(pred, lambda: copy(name, dst, dst, across).wait_recv())

    def img(ref, k):
        return ref.block(k)

    class Split:
        def __init__(self, make):
            self.copies = [make(b, pl.ds(b * LANES, LANES)) for b in range(HALVES)]

        def start(self):
            for one in self.copies:
                one.start()

        def wait(self):
            for one in self.copies:
                one.wait()

    own_in = [
        Split(lambda b, cols, j=j: pltpu.make_async_copy(vol.at[0, j, :, cols], OWN.at[1 + j, b], ls.at[j, b]))
        for j in range(NZ)
    ]
    for j in (0, 3, 1, 2):
        own_in[j].start()

    barrier = pltpu.get_barrier_semaphore()
    for target, pred in ((plus, None), (minus, None), (across, None), (below, has_below), (above, has_above)):
        when(pred, lambda target=target: pl.semaphore_signal(barrier, inc=1, device_id=target, device_id_type=MESH))
    dual_in = Split(lambda b, cols: pltpu.make_async_copy(dua.at[0, :, :, :, cols], DU.at[:, :, b], ls.at[4, b]))
    prior_in = Split(lambda b, cols: pltpu.make_async_copy(pri.at[0, :, :, cols], PRI.at[:, b], ls.at[5, b]))
    pl.semaphore_wait(barrier, 3 + has_below.astype(jnp.int32) + has_above.astype(jnp.int32))

    not_p3 = pos < 3
    not_p0 = pos > 0
    not_first, not_last = jnp.logical_not(first), jnp.logical_not(last)

    def send_own(sign, j):
        src = OWN.at[1 + j]
        if sign > 0:
            name, target, inside, edge, spare, into = ("P", j), plus, not_p3, pos == 3, last, img(R3, 1 + j)
            direct = j >= 2
        else:
            name, target, inside, edge, spare, into = ("M", j), minus, not_p0, pos == 0, first, img(R1, 1 + j)
            direct = j < 2
        send(name, src, into, target, inside)
        if direct:
            arrive(("XV", j), V.at[j], spare)
            send(name, V.at[j], into, target, spare)
        else:
            send(name, src, W.at[j], target, edge)

    def send_across():
        for j in (3, 2):
            send(("XV", j), OWN.at[1 + j], V.at[j], across, c == 3)
        for j in (0, 1):
            send(("XV", j), OWN.at[1 + j], V.at[j], across, c == 4)

    def halo(i, ref, k, src=None, pred=None):
        own = ref is OWN
        at = (lambda k: ref.at[k]) if own else (lambda k: img(ref, k))
        both = lambda a: a if pred is None else jnp.logical_and(a, pred)
        if k == 1:
            send(("HL", i), at(1), at(5), below, both(has_below))
        else:
            send(("HH", i), at(4), at(0), above, both(has_above))

    def halo_arrive(i, ref, pred=None):
        own = ref is OWN
        at = (lambda k: ref.at[k]) if own else (lambda k: img(ref, k))
        both = lambda a: a if pred is None else jnp.logical_and(a, pred)
        arrive(("HL", i), at(5), both(has_above))
        arrive(("HH", i), at(0), both(has_below))

    own_in[0].wait()
    send_own(1, 0)
    own_in[3].wait()
    send_own(-1, 3)
    own_in[1].wait()
    send_own(1, 1)
    own_in[2].wait()
    send_own(-1, 2)
    send_across()
    halo(0, OWN, 1)
    halo(0, OWN, 4)
    dual_in.start()
    prior_in.start()

    zeros = jnp.zeros((6, HALVES, PAD, LANES), jnp.float32)
    for ref in (R1.main, R3.main, R2.main, X2.main):
        ref[:, :, pl.ds(0, PAD), :] = zeros
        ref[:, :, pl.ds(PAD + NY, PAD), :] = zeros
    for ref in (Z, FL, R1L, R3L):
        ref[:, pl.ds(0, PAD), :] = zeros[0]
        ref[:, pl.ds(PAD + NY, PAD), :] = zeros[0]

    @pl.when(s == 0)
    def _():
        for sums in (T, T1, T3):
            sums[0] = jnp.zeros((HALVES, NY, LANES), jnp.float32)

    @pl.when(s == 3)
    def _():
        for sums in (T, T1, T3):
            sums[5] = jnp.zeros((HALVES, NY, LANES), jnp.float32)

    def got_plus(j):
        if j < 2:
            arrive(("P", j), img(R3, 1 + j), not_p0)
            arrive(("P", j), W.at[j], pos == 0)
            send(("PR", j), img(R3, 1 + j), img(R2, 1 + j), plus, not_p0)
            send(("PR", j), W.at[j], img(R2, 1 + j), plus, pos == 0)
            send(("XW", j), W.at[j], img(R3, 1 + j), across, first)
            if j == 0:
                halo(2, R3, 1, pred=not_p0)
        else:
            arrive(("P", j), img(R3, 1 + j), not_first)
            if j == 3:
                halo(2, R3, 4, pred=not_first)

    def got_minus(j):
        if j >= 2:
            arrive(("M", j), img(R1, 1 + j), not_p3)
            arrive(("M", j), W.at[j], pos == 3)
            send(("MR", j), img(R1, 1 + j), img(R2, 1 + j), minus, not_p3)
            send(("MR", j), W.at[j], img(R2, 1 + j), minus, pos == 3)
            send(("XW", j), W.at[j], img(R1, 1 + j), across, last)
            if j == 3:
                halo(1, R1, 4, pred=not_p3)
        else:
            arrive(("M", j), img(R1, 1 + j), not_last)
            if j == 0:
                halo(1, R1, 1, pred=not_last)

    up = (0, 1, 3, 2)
    down = (3, 2, 0, 1)

    def own(rank):
        send_own(1, up[rank])
        send_own(-1, down[rank])

    def got(rank):
        got_plus(up[rank])
        got_minus(down[rank])

    def got_opposite(name, j):
        arrive((name, j), img(R2, 1 + j))
        send(("XO", j), img(R2, 1 + j), img(X2, 1 + j), across, outer)
        if j in (0, 3):
            halo(3, R2, 1 + j)

    lane = lax.broadcasted_iota(jnp.int32, (CHUNK, LANES), 1)
    left, right = lane == 0, lane == LANES - 1
    k_lo = 1 - has_below.astype(jnp.int32)
    k_hi = 5 + has_above.astype(jnp.int32)
    chunks = NY // CHUNK

    def pair(p, direction, ref, out, fresh_sum, T):
        slot = jnp.int32(0)
        shift = jnp.int32(0)
        active = jnp.int32(0)
        for k in range(4):
            hit = cyc[0, k] == direction
            slot = slot + jnp.where(hit, k, 0)
            shift = shift + jnp.where(hit, off[0, k], 0)
            active = active + jnp.where(hit, 1, 0)
        live = active > 0

        def contrast(k, b, r):
            return ref.load(k, b, PAD - shift + r) - OWN[k, b, pl.ds(r, CHUNK), :]

        def squares(k):
            for q in range(chunks):
                r = q * CHUNK
                x0, x1 = contrast(k, 0, r), contrast(k, 1, r)
                x0, x1 = x0 * x0, x1 * x1
                l0, l1 = pltpu.roll(x0, 1, 1), pltpu.roll(x1, 1, 1)
                r0, r1 = pltpu.roll(x0, LANES - 1, 1), pltpu.roll(x1, LANES - 1, 1)
                T[k, 0, pl.ds(r, CHUNK), :] = x0 + jnp.where(left, 0.0, l0) + jnp.where(right, r1, r0)
                T[k, 1, pl.ds(r, CHUNK), :] = x1 + jnp.where(left, l0, l1) + jnp.where(right, 0.0, r1)

        def update(j):
            for b in range(HALVES):
                for q in range(chunks):
                    rows = pl.ds(q * CHUNK, CHUNK)
                    Z[b, pl.ds(PAD + q * CHUNK, CHUNK), :] = T[j, b, rows, :] + T[j + 1, b, rows, :] + T[j + 2, b, rows, :]
                for q in range(chunks):
                    r = q * CHUNK
                    rows = pl.ds(r, CHUNK)
                    total = (
                        Z[b, pl.ds(PAD - 1 + r, CHUNK), :]
                        + Z[b, pl.ds(PAD + r, CHUNK), :]
                        + Z[b, pl.ds(PAD + 1 + r, CHUNK), :]
                    )
                    w = jnp.exp(total * (-1.0 / 108.0))
                    fresh = jnp.clip(DU[slot, j, b, rows, :] + 0.5 * w * contrast(j + 1, b, r), -0.3, 0.3)
                    fresh = jnp.where(live, fresh, 0.0)
                    FR[p, j, b, rows, :] = fresh
                    flux = w * fresh
                    if fresh_sum:
                        LS[j, b, rows, :] = flux
                    else:
                        LS[j, b, rows, :] = LS[j, b, rows, :] + flux
                    FL[b, pl.ds(PAD + r, CHUNK), :] = flux
                for q in range(chunks):
                    r = q * CHUNK
                    out[j, b, pl.ds(r, CHUNK), :] = FL[b, pl.ds(PAD + shift + r, CHUNK), :]

        return squares, update

    def all_squares(squares):
        def one(k, carry):
            squares(k)
            return carry

        lax.fori_loop(k_lo, k_hi, one, 0)

    def updates(update, order, emit):
        for n, j in enumerate(order):
            update(j)
            if n > 0:
                emit(order[n - 1])
        emit(order[-1])

    forward = pos < 2
    def opposite(rank):
        got_opposite("PR", rank)
        got_opposite("MR", 3 - rank)

    def send_far(pred, j):
        if j < 2:
            send(("PF", j), F2.at[j], RP.at[j], plus, pred)
        else:
            send(("MF", j), F2.at[j], RM.at[j - 2], minus, pred)

    def pair_far():
        halo_arrive(3, R2)
        squares, update = pair(2, jnp.where(forward, 2, -2), R2, F2, True, T)
        all_squares(squares)
        updates(update, (0, 3, 1, 2), functools.partial(send_far, inner))

    def pair_across():
        for j in (0, 3, 1, 2):
            arrive(("XO", j), img(X2, 1 + j), inner)
            if j in (0, 3):
                halo(4, X2, 1 + j, pred=inner)
        halo_arrive(4, X2, inner)

        def emit(j):
            send(("FO", j), FX.at[j], XF2.at[j], across, inner)

        @pl.when(inner)
        def _():
            squares, update = pair(3, jnp.where(forward, -2, 2), X2, FX, False, T)
            all_squares(squares)
            updates(update, (0, 3, 1, 2), emit)

    def got_across():
        for j in (3, 2):
            arrive(("XW", j), img(R1, 1 + j), c == 3)
        halo(1, R1, 4, pred=c == 3)
        for j in (0, 1):
            arrive(("XW", j), img(R3, 1 + j), c == 4)
        halo(2, R3, 1, pred=c == 4)

    next_squares, next_update = pair(0, 1, R1, F1P, False, T1)
    before_squares, before_update = pair(1, -1, R3, F1M, False, T3)

    def next_emit(j):
        if j < 2:
            send(("FX", j), F1P.at[j], XF1.at[j], across, is3)
        else:
            send(("PD", j), F1P.at[j], INM.at[j], plus, not_last)

    def before_emit(j):
        if j < 2:
            send(("MD", j), F1M.at[j], INP.at[j], minus, not_first)
        else:
            send(("FX", j), F1M.at[j], XF1.at[j], across, is4)

    def early():
        halo_arrive(1, R1, not_last)

        @pl.when(not_last)
        def _():
            pl.when(has_above)(functools.partial(next_squares, 5))
            next_squares(4)
            next_squares(3)
            next_update(3)

        halo_arrive(2, R3, not_first)

        @pl.when(not_first)
        def _():
            pl.when(has_below)(functools.partial(before_squares, 0))
            before_squares(1)
            before_squares(2)
            before_update(0)

        next_emit(3)
        before_emit(0)

        @pl.when(not_last)
        def _():
            pl.when(has_below)(functools.partial(next_squares, 0))
            next_squares(1)

        @pl.when(not_first)
        def _():
            pl.when(has_above)(functools.partial(before_squares, 5))
            before_squares(4)

    def late():
        @pl.when(not_last)
        def _():
            next_squares(2)
            next_update(2)

        @pl.when(not_first)
        def _():
            before_squares(3)
            before_update(1)

        next_emit(2)
        before_emit(1)

        @pl.when(not_last)
        def _():
            updates(next_update, (0, 1), next_emit)

        @pl.when(not_first)
        def _():
            updates(before_update, (3, 2), before_emit)

    def far_outer():
        for j in (0, 3, 1, 2):
            arrive(("FO", j), XF2.at[j], outer)

            @pl.when(outer)
            def _():
                F2[j] = F2[j] + XF2[j]

            if j == 0 or j == 1:
                send(("PF", j), F2.at[j], RP.at[j], plus, outer)
            else:
                send(("MF", j), F2.at[j], RM.at[j - 2], minus, outer)

    halo_arrive(0, OWN)
    dual_in.wait()
    got(0)
    own(2)
    got(1)
    own(3)
    opposite(0)
    opposite(1)
    pair_far()
    got(2)
    pair_across()
    got_across()
    early()
    got(3)
    late()
    far_outer()

    for j in (0, 1):
        arrive(("FX", j), XF1.at[j], last)
    for j in (3, 2):
        arrive(("FX", j), XF1.at[j], first)

    def pass_on():
        for j in (3, 2):
            arrive(("PD", j), INM.at[j], first)
            send(("XD", j), INM.at[j], INM.at[j], across, first)
        for j in (0, 1):
            arrive(("MD", j), INP.at[j], last)
            send(("XD", j), INP.at[j], INP.at[j], across, last)

    def slot_out(k):
        cycle = cyc[0, k]
        hop = jnp.where(cycle > 0, 0, 1)
        far = jnp.where((cycle > 0) == forward, 2, 3)
        p = jnp.where(jnp.logical_or(cycle == 1, cycle == -1), hop, far)

        def put(j, carry):
            DU[k, j] = jnp.where(cycle != 0, FR[p, j], 0.0)
            return carry

        lax.fori_loop(0, NZ, put, 0)

    for k in range(4):
        slot_out(k)
    dual_out = Split(lambda b, cols: pltpu.make_async_copy(DU.at[:, :, b], dn_out.at[0, :, :, :, cols], ls.at[6, b]))
    dual_out.start()
    prior_in.wait()

    def start_volume(j, carry):
        VN[j] = OWN[1 + j] + 0.25 * LS[j] + 0.25 * PRI[j]
        return carry

    lax.fori_loop(0, NZ, start_volume, 0)

    def second(name, onward, rel, sums, base, spare, j, i, target, none, swap, dst):
        arrive((name, j), rel.at[i])

        @pl.when(none)
        def _():
            sums[i] = rel[i]

        @pl.when(swap)
        def _():
            sums[i] = rel[i] + spare[j]

        @pl.when(jnp.logical_not(jnp.logical_or(none, swap)))
        def _():
            sums[i] = rel[i] + base[j]

        send((onward, j), sums.at[i], dst.at[j], target)

    second("PF", "PS", RP, SP, F1P, XF1, 0, 0, plus, c == 3, last, INM)
    second("MF", "MS", RM, SM, F1M, XF1, 3, 1, minus, c == 4, first, INP)
    pass_on()
    second("PF", "PS", RP, SP, F1P, XF1, 1, 1, plus, c == 3, last, INM)
    second("MF", "MS", RM, SM, F1M, XF1, 2, 0, minus, c == 4, first, INP)

    def take(ref, j):
        VN[j] = VN[j] - 0.25 * ref[j]

    for j in (2, 3):
        arrive(("PD", j), INM.at[j], jnp.logical_and(c != 4, not_first))
        arrive(("XD", j), INM.at[j], c == 4)
        pl.when(not_first)(functools.partial(take, INM, j))
    for j in (1, 0):
        arrive(("MD", j), INP.at[j], jnp.logical_and(c != 3, not_last))
        arrive(("XD", j), INP.at[j], c == 3)
        pl.when(not_last)(functools.partial(take, INP, j))

    for name, ref, j in (("PS", INM, 0), ("MS", INP, 3), ("PS", INM, 1), ("MS", INP, 2)):
        arrive((name, j), ref.at[j])
        for b in range(HALVES):
            vn_out[0, j, :, pl.ds(b * LANES, LANES)] = (VN[j, b] - 0.25 * ref[j, b]) / 1.25

    for name, target, pred in sent:
        when(pred, lambda: copy(name, OWN.at[0], OWN.at[0], target).wait_send())
    dual_out.wait()


def results(volume_in, dual_in, volume_out, dual_out, sems):
    copies = []
    for k in range(4):
        for half in range(2):
            rows = pl.ds(2 * half, 2)
            copies.append(pltpu.make_async_copy(dual_in.at[0, k, rows], dual_out.at[0, k, rows], sems.at[k, half]))
    for half in range(2):
        rows = pl.ds(2 * half, 2)
        copies.append(pltpu.make_async_copy(volume_in.at[0, rows], volume_out.at[0, rows], sems.at[4, half]))
    for one in copies:
        one.start()
    for one in copies:
        one.wait()


def shards(volume, prior_image, dual_pairs, pair_cycle, pair_offset):
    image = pltpu.VMEM((NZ + 2, HALVES, ROWS, LANES), jnp.float32)
    block = pltpu.VMEM((NZ, HALVES, NY, LANES), jnp.float32)
    half = pltpu.VMEM((2, HALVES, NY, LANES), jnp.float32)
    plane = pltpu.VMEM((HALVES, ROWS, LANES), jnp.float32)
    stack = pltpu.VMEM((NZ + 2, HALVES, NY, LANES), jnp.float32)
    slots = pltpu.VMEM((4, NZ, HALVES, NY, LANES), jnp.float32)
    smem = pl.BlockSpec(memory_space=pltpu.SMEM)
    anyspace = pl.BlockSpec(memory_space=pl.ANY)
    volume_next, dual_next = pl.pallas_call(
        kernel,
        out_shape=(
            pltpu.VMEM(volume.shape, jnp.float32),
            pltpu.VMEM(dual_pairs.shape, jnp.float32),
        ),
        in_specs=[smem, smem, anyspace, anyspace, anyspace],
        out_specs=(pl.BlockSpec(memory_space=pltpu.VMEM), anyspace),
        scratch_shapes=[
            stack, image, image, image, image, plane, plane, block, block,
            stack, stack, stack, plane, plane, slots, slots,
            block, block, block, block, block, block,
            half, half, half, half, block, block,
            block, block, block,
            pltpu.SemaphoreType.DMA((len(NAMES),)),
            pltpu.SemaphoreType.DMA((len(NAMES),)),
            pltpu.SemaphoreType.DMA((7, HALVES)),
        ],
        compiler_params=pltpu.CompilerParams(collective_id=0, vmem_limit_bytes=61_790_000, has_side_effects=True),
    )(pair_cycle, pair_offset, volume, prior_image, dual_pairs)
    return pl.pallas_call(
        results,
        out_shape=(
            jax.ShapeDtypeStruct(volume.shape, jnp.float32),
            jax.ShapeDtypeStruct(dual_pairs.shape, jnp.float32),
        ),
        in_specs=[anyspace, anyspace],
        out_specs=(anyspace, anyspace),
        scratch_shapes=[pltpu.SemaphoreType.DMA((5, 2))],
        compiler_params=pltpu.CompilerParams(vmem_limit_bytes=1024 * 1024),
    )(volume_next, dual_next)


def solution(mesh):
    return jax.shard_map(
        shards,
        mesh=mesh,
        in_specs=(
            P("tm", "space", None, None),
            P("tm", "space", None, None),
            P("tm", None, "space", None, None),
            P("tm", None),
            P("tm", None),
        ),
        out_specs=(P("tm", "space", None, None), P("tm", None, "space", None, None)),
        check_vma=False,
    )
```

```python
import functools

import jax
import jax.numpy as jnp
from jax import lax
from jax.experimental import pallas as pl
from jax.experimental.pallas import tpu as pltpu
from jax.sharding import PartitionSpec as P

MESH = pl.DeviceIdType.MESH

NZ, NY = 4, 256
LANES, HALVES = 128, 2
PAD = 8
ROWS = NY + 2 * PAD
CHUNK = 64

NAMES = []
for stem, slices in (
    ("P", (0, 1, 2, 3)),
    ("M", (0, 1, 2, 3)),
    ("PR", (0, 1)),
    ("MR", (2, 3)),
    ("XW", (0, 1, 2, 3)),
    ("XO", (0, 1, 2, 3)),
    ("XV", (0, 1, 2, 3)),
    ("HL", (0, 1, 2, 3, 4)),
    ("HH", (0, 1, 2, 3, 4)),
    ("FX", (0, 1, 2, 3)),
    ("XD", (0, 1, 2, 3)),
    ("FO", (0, 1, 2, 3)),
    ("PD", (2, 3)),
    ("MD", (0, 1)),
    ("PF", (0, 1)),
    ("MF", (2, 3)),
    ("PS", (0, 1)),
    ("MS", (2, 3)),
):
    NAMES += [(stem, j) for j in slices]
SEM = {name: i for i, name in enumerate(NAMES)}


def when(pred, fn):
    if pred is None:
        fn()
    else:
        pl.when(pred)(fn)


class Image:
    def __init__(self, main, late=None, late_k=None):
        self.main, self.late, self.late_k = main, late, late_k

    def block(self, k):
        if self.late is not None and k == self.late_k:
            return self.late.at[:, pl.ds(PAD, NY), :]
        return self.main.at[k, :, pl.ds(PAD, NY), :]

    def load(self, k, b, start):
        if self.late is not None and k == self.late_k:
            return self.late[b, pl.ds(start, CHUNK), :]
        return self.main[k, b, pl.ds(start, CHUNK), :]


def kernel(
    cyc, off, vol, pri, dua, vn_out, dn_out,
    OWN, R1, R3, R2, X2, R1L, R3L, W, V, T, T1, T3, Z, FL, DU, FR, F1P, F1M, F2, FX, XF1, XF2,
    RP, RM, SP, SM, INM, INP, LS, PRI, VN, ss, rs, ls,
):
    R1, R3, R2, X2 = Image(R1, R1L, 2), Image(R3, R3L, 3), Image(R2), Image(X2)
    tm = lax.axis_index("tm")
    s = lax.axis_index("space")
    h = tm // 32
    z = (tm // 4) % 8
    y = tm % 4
    pos = z // 2
    c = 4 * h + pos
    plus = (h * 32 + ((z + 2) % 8) * 4 + y, s)
    minus = (h * 32 + ((z + 6) % 8) * 4 + y, s)
    across = ((1 - h) * 32 + z * 4 + y, s)
    below = (tm, lax.max(s - 1, 0))
    above = (tm, lax.min(s + 1, 3))
    has_below = s > 0
    has_above = s < 3
    first, last = c == 0, c == 7
    is3, is4 = c == 3, c == 4
    inner = jnp.logical_and(c > 1, c < 6)
    outer = jnp.logical_not(inner)

    def copy(name, src, dst, target):
        i = SEM[name]
        return pltpu.make_async_remote_copy(
            src_ref=src, dst_ref=dst, send_sem=ss.at[i], recv_sem=rs.at[i],
            device_id=target, device_id_type=MESH,
        )

    sent = []

    def send(name, src, dst, target, pred=None):
        when(pred, lambda: copy(name, src, dst, target).start())
        sent.append((name, target, pred))

    def arrive(name, dst, pred=None):
        when(pred, lambda: copy(name, dst, dst, across).wait_recv())

    def img(ref, k):
        return ref.block(k)

    class Split:
        def __init__(self, make):
            self.copies = [make(b, pl.ds(b * LANES, LANES)) for b in range(HALVES)]

        def start(self):
            for one in self.copies:
                one.start()

        def wait(self):
            for one in self.copies:
                one.wait()

    own_in = [
        Split(lambda b, cols, j=j: pltpu.make_async_copy(vol.at[0, j, :, cols], OWN.at[1 + j, b], ls.at[j, b]))
        for j in range(NZ)
    ]
    for j in (0, 3, 1, 2):
        own_in[j].start()

    barrier = pltpu.get_barrier_semaphore()
    for target, pred in ((plus, None), (minus, None), (across, None), (below, has_below), (above, has_above)):
        when(pred, lambda target=target: pl.semaphore_signal(barrier, inc=1, device_id=target, device_id_type=MESH))
    dual_in = Split(lambda b, cols: pltpu.make_async_copy(dua.at[0, :, :, :, cols], DU.at[:, :, b], ls.at[4, b]))
    prior_in = Split(lambda b, cols: pltpu.make_async_copy(pri.at[0, :, :, cols], PRI.at[:, b], ls.at[5, b]))
    pl.semaphore_wait(barrier, 3 + has_below.astype(jnp.int32) + has_above.astype(jnp.int32))

    not_p3 = pos < 3
    not_p0 = pos > 0
    not_first, not_last = jnp.logical_not(first), jnp.logical_not(last)

    def send_own(sign, j):
        src = OWN.at[1 + j]
        if sign > 0:
            name, target, inside, edge, spare, into = ("P", j), plus, not_p3, pos == 3, last, img(R3, 1 + j)
            direct = j >= 2
        else:
            name, target, inside, edge, spare, into = ("M", j), minus, not_p0, pos == 0, first, img(R1, 1 + j)
            direct = j < 2
        send(name, src, into, target, inside)
        if direct:
            arrive(("XV", j), V.at[j], spare)
            send(name, V.at[j], into, target, spare)
        else:
            send(name, src, W.at[j], target, edge)

    def send_across():
        for j in (3, 2):
            send(("XV", j), OWN.at[1 + j], V.at[j], across, c == 3)
        for j in (0, 1):
            send(("XV", j), OWN.at[1 + j], V.at[j], across, c == 4)

    def halo(i, ref, k, src=None, pred=None):
        own = ref is OWN
        at = (lambda k: ref.at[k]) if own else (lambda k: img(ref, k))
        both = lambda a: a if pred is None else jnp.logical_and(a, pred)
        if k == 1:
            send(("HL", i), at(1), at(5), below, both(has_below))
        else:
            send(("HH", i), at(4), at(0), above, both(has_above))

    def halo_arrive(i, ref, pred=None):
        own = ref is OWN
        at = (lambda k: ref.at[k]) if own else (lambda k: img(ref, k))
        both = lambda a: a if pred is None else jnp.logical_and(a, pred)
        arrive(("HL", i), at(5), both(has_above))
        arrive(("HH", i), at(0), both(has_below))

    own_in[0].wait()
    send_own(1, 0)
    own_in[3].wait()
    send_own(-1, 3)
    own_in[1].wait()
    send_own(1, 1)
    own_in[2].wait()
    send_own(-1, 2)
    send_across()
    halo(0, OWN, 1)
    halo(0, OWN, 4)
    dual_in.start()
    prior_in.start()

    zeros = jnp.zeros((6, HALVES, PAD, LANES), jnp.float32)
    for ref in (R1.main, R3.main, R2.main, X2.main):
        ref[:, :, pl.ds(0, PAD), :] = zeros
        ref[:, :, pl.ds(PAD + NY, PAD), :] = zeros
    for ref in (Z, FL, R1L, R3L):
        ref[:, pl.ds(0, PAD), :] = zeros[0]
        ref[:, pl.ds(PAD + NY, PAD), :] = zeros[0]

    @pl.when(s == 0)
    def _():
        for sums in (T, T1, T3):
            sums[0] = jnp.zeros((HALVES, NY, LANES), jnp.float32)

    @pl.when(s == 3)
    def _():
        for sums in (T, T1, T3):
            sums[5] = jnp.zeros((HALVES, NY, LANES), jnp.float32)

    def got_plus(j):
        if j < 2:
            arrive(("P", j), img(R3, 1 + j), not_p0)
            arrive(("P", j), W.at[j], pos == 0)
            send(("PR", j), img(R3, 1 + j), img(R2, 1 + j), plus, not_p0)
            send(("PR", j), W.at[j], img(R2, 1 + j), plus, pos == 0)
            send(("XW", j), W.at[j], img(R3, 1 + j), across, first)
            if j == 0:
                halo(2, R3, 1, pred=not_p0)
        else:
            arrive(("P", j), img(R3, 1 + j), not_first)
            if j == 3:
                halo(2, R3, 4, pred=not_first)

    def got_minus(j):
        if j >= 2:
            arrive(("M", j), img(R1, 1 + j), not_p3)
            arrive(("M", j), W.at[j], pos == 3)
            send(("MR", j), img(R1, 1 + j), img(R2, 1 + j), minus, not_p3)
            send(("MR", j), W.at[j], img(R2, 1 + j), minus, pos == 3)
            send(("XW", j), W.at[j], img(R1, 1 + j), across, last)
            if j == 3:
                halo(1, R1, 4, pred=not_p3)
        else:
            arrive(("M", j), img(R1, 1 + j), not_last)
            if j == 0:
                halo(1, R1, 1, pred=not_last)

    up = (0, 1, 3, 2)
    down = (3, 2, 0, 1)

    def own(rank):
        send_own(1, up[rank])
        send_own(-1, down[rank])

    def got(rank):
        got_plus(up[rank])
        got_minus(down[rank])

    def got_opposite(name, j):
        arrive((name, j), img(R2, 1 + j))
        send(("XO", j), img(R2, 1 + j), img(X2, 1 + j), across, outer)
        if j in (0, 3):
            halo(3, R2, 1 + j)

    lane = lax.broadcasted_iota(jnp.int32, (CHUNK, LANES), 1)
    left, right = lane == 0, lane == LANES - 1
    k_lo = 1 - has_below.astype(jnp.int32)
    k_hi = 5 + has_above.astype(jnp.int32)
    chunks = NY // CHUNK

    def pair(p, direction, ref, out, fresh_sum, T):
        slot = jnp.int32(0)
        shift = jnp.int32(0)
        active = jnp.int32(0)
        for k in range(4):
            hit = cyc[0, k] == direction
            slot = slot + jnp.where(hit, k, 0)
            shift = shift + jnp.where(hit, off[0, k], 0)
            active = active + jnp.where(hit, 1, 0)
        live = active > 0

        def contrast(k, b, r):
            return ref.load(k, b, PAD - shift + r) - OWN[k, b, pl.ds(r, CHUNK), :]

        def squares(k):
            for q in range(chunks):
                r = q * CHUNK
                x0, x1 = contrast(k, 0, r), contrast(k, 1, r)
                x0, x1 = x0 * x0, x1 * x1
                l0, l1 = pltpu.roll(x0, 1, 1), pltpu.roll(x1, 1, 1)
                r0, r1 = pltpu.roll(x0, LANES - 1, 1), pltpu.roll(x1, LANES - 1, 1)
                T[k, 0, pl.ds(r, CHUNK), :] = x0 + jnp.where(left, 0.0, l0) + jnp.where(right, r1, r0)
                T[k, 1, pl.ds(r, CHUNK), :] = x1 + jnp.where(left, l0, l1) + jnp.where(right, 0.0, r1)

        def update(j):
            for b in range(HALVES):
                for q in range(chunks):
                    rows = pl.ds(q * CHUNK, CHUNK)
                    Z[b, pl.ds(PAD + q * CHUNK, CHUNK), :] = T[j, b, rows, :] + T[j + 1, b, rows, :] + T[j + 2, b, rows, :]
                for q in range(chunks):
                    r = q * CHUNK
                    rows = pl.ds(r, CHUNK)
                    total = (
                        Z[b, pl.ds(PAD - 1 + r, CHUNK), :]
                        + Z[b, pl.ds(PAD + r, CHUNK), :]
                        + Z[b, pl.ds(PAD + 1 + r, CHUNK), :]
                    )
                    w = jnp.exp(total * (-1.0 / 108.0))
                    fresh = jnp.clip(DU[slot, j, b, rows, :] + 0.5 * w * contrast(j + 1, b, r), -0.3, 0.3)
                    fresh = jnp.where(live, fresh, 0.0)
                    FR[p, j, b, rows, :] = fresh
                    flux = w * fresh
                    if fresh_sum:
                        LS[j, b, rows, :] = flux
                    else:
                        LS[j, b, rows, :] = LS[j, b, rows, :] + flux
                    FL[b, pl.ds(PAD + r, CHUNK), :] = flux
                for q in range(chunks):
                    r = q * CHUNK
                    out[j, b, pl.ds(r, CHUNK), :] = FL[b, pl.ds(PAD + shift + r, CHUNK), :]

        return squares, update

    def all_squares(squares):
        def one(k, carry):
            squares(k)
            return carry

        lax.fori_loop(k_lo, k_hi, one, 0)

    def updates(update, order, emit):
        for n, j in enumerate(order):
            update(j)
            if n > 0:
                emit(order[n - 1])
        emit(order[-1])

    forward = pos < 2
    def opposite(rank):
        got_opposite("PR", rank)
        got_opposite("MR", 3 - rank)

    def send_far(pred, j):
        if j < 2:
            send(("PF", j), F2.at[j], RP.at[j], plus, pred)
        else:
            send(("MF", j), F2.at[j], RM.at[j - 2], minus, pred)

    def pair_far():
        halo_arrive(3, R2)
        squares, update = pair(2, jnp.where(forward, 2, -2), R2, F2, True, T)
        all_squares(squares)
        updates(update, (0, 3, 1, 2), functools.partial(send_far, inner))

    def pair_across():
        for j in (0, 3, 1, 2):
            arrive(("XO", j), img(X2, 1 + j), inner)
            if j in (0, 3):
                halo(4, X2, 1 + j, pred=inner)
        halo_arrive(4, X2, inner)

        def emit(j):
            send(("FO", j), FX.at[j], XF2.at[j], across, inner)

        @pl.when(inner)
        def _():
            squares, update = pair(3, jnp.where(forward, -2, 2), X2, FX, False, T)
            all_squares(squares)
            updates(update, (0, 3, 1, 2), emit)

    def got_across():
        for j in (3, 2):
            arrive(("XW", j), img(R1, 1 + j), c == 3)
        halo(1, R1, 4, pred=c == 3)
        for j in (0, 1):
            arrive(("XW", j), img(R3, 1 + j), c == 4)
        halo(2, R3, 1, pred=c == 4)

    next_squares, next_update = pair(0, 1, R1, F1P, False, T1)
    before_squares, before_update = pair(1, -1, R3, F1M, False, T3)

    def next_emit(j):
        if j < 2:
            send(("FX", j), F1P.at[j], XF1.at[j], across, is3)
        else:
            send(("PD", j), F1P.at[j], INM.at[j], plus, not_last)

    def before_emit(j):
        if j < 2:
            send(("MD", j), F1M.at[j], INP.at[j], minus, not_first)
        else:
            send(("FX", j), F1M.at[j], XF1.at[j], across, is4)

    def early():
        halo_arrive(1, R1, not_last)

        @pl.when(not_last)
        def _():
            pl.when(has_above)(functools.partial(next_squares, 5))
            next_squares(4)
            next_squares(3)
            next_update(3)

        halo_arrive(2, R3, not_first)

        @pl.when(not_first)
        def _():
            pl.when(has_below)(functools.partial(before_squares, 0))
            before_squares(1)
            before_squares(2)
            before_update(0)

        next_emit(3)
        before_emit(0)

        @pl.when(not_last)
        def _():
            pl.when(has_below)(functools.partial(next_squares, 0))
            next_squares(1)

        @pl.when(not_first)
        def _():
            pl.when(has_above)(functools.partial(before_squares, 5))
            before_squares(4)

    def late():
        @pl.when(not_last)
        def _():
            next_squares(2)
            next_update(2)

        @pl.when(not_first)
        def _():
            before_squares(3)
            before_update(1)

        next_emit(2)
        before_emit(1)

        @pl.when(not_last)
        def _():
            updates(next_update, (0, 1), next_emit)

        @pl.when(not_first)
        def _():
            updates(before_update, (3, 2), before_emit)

    def far_outer():
        for j in (0, 3, 1, 2):
            arrive(("FO", j), XF2.at[j], outer)

            @pl.when(outer)
            def _():
                F2[j] = F2[j] + XF2[j]

            if j == 0 or j == 1:
                send(("PF", j), F2.at[j], RP.at[j], plus, outer)
            else:
                send(("MF", j), F2.at[j], RM.at[j - 2], minus, outer)

    halo_arrive(0, OWN)
    dual_in.wait()
    got(0)
    own(2)
    got(1)
    own(3)
    opposite(0)
    opposite(1)
    pair_far()
    got(2)
    pair_across()
    got_across()
    early()
    got(3)
    late()
    far_outer()

    for j in (0, 1):
        arrive(("FX", j), XF1.at[j], last)
    for j in (3, 2):
        arrive(("FX", j), XF1.at[j], first)

    def pass_on():
        for j in (3, 2):
            arrive(("PD", j), INM.at[j], first)
            send(("XD", j), INM.at[j], INM.at[j], across, first)
        for j in (0, 1):
            arrive(("MD", j), INP.at[j], last)
            send(("XD", j), INP.at[j], INP.at[j], across, last)

    def slot_out(k):
        cycle = cyc[0, k]
        hop = jnp.where(cycle > 0, 0, 1)
        far = jnp.where((cycle > 0) == forward, 2, 3)
        p = jnp.where(jnp.logical_or(cycle == 1, cycle == -1), hop, far)

        def put(j, carry):
            DU[k, j] = jnp.where(cycle != 0, FR[p, j], 0.0)
            return carry

        lax.fori_loop(0, NZ, put, 0)

    for k in range(4):
        slot_out(k)
    dual_out = Split(lambda b, cols: pltpu.make_async_copy(DU.at[:, :, b], dn_out.at[0, :, :, :, cols], ls.at[6, b]))
    dual_out.start()
    prior_in.wait()

    def start_volume(j, carry):
        VN[j] = OWN[1 + j] + 0.25 * LS[j] + 0.25 * PRI[j]
        return carry

    lax.fori_loop(0, NZ, start_volume, 0)

    def second(name, onward, rel, sums, base, spare, j, i, target, none, swap, dst):
        arrive((name, j), rel.at[i])

        @pl.when(none)
        def _():
            sums[i] = rel[i]

        @pl.when(swap)
        def _():
            sums[i] = rel[i] + spare[j]

        @pl.when(jnp.logical_not(jnp.logical_or(none, swap)))
        def _():
            sums[i] = rel[i] + base[j]

        send((onward, j), sums.at[i], dst.at[j], target)

    second("PF", "PS", RP, SP, F1P, XF1, 0, 0, plus, c == 3, last, INM)
    second("MF", "MS", RM, SM, F1M, XF1, 3, 1, minus, c == 4, first, INP)
    pass_on()
    second("PF", "PS", RP, SP, F1P, XF1, 1, 1, plus, c == 3, last, INM)
    second("MF", "MS", RM, SM, F1M, XF1, 2, 0, minus, c == 4, first, INP)

    def take(ref, j):
        VN[j] = VN[j] - 0.25 * ref[j]

    for j in (2, 3):
        arrive(("PD", j), INM.at[j], jnp.logical_and(c != 4, not_first))
        arrive(("XD", j), INM.at[j], c == 4)
        pl.when(not_first)(functools.partial(take, INM, j))
    for j in (1, 0):
        arrive(("MD", j), INP.at[j], jnp.logical_and(c != 3, not_last))
        arrive(("XD", j), INP.at[j], c == 3)
        pl.when(not_last)(functools.partial(take, INP, j))

    for name, ref, j in (("PS", INM, 0), ("MS", INP, 3), ("PS", INM, 1), ("MS", INP, 2)):
        arrive((name, j), ref.at[j])
        for b in range(HALVES):
            vn_out[0, j, :, pl.ds(b * LANES, LANES)] = (VN[j, b] - 0.25 * ref[j, b]) / 1.25

    for name, target, pred in sent:
        when(pred, lambda: copy(name, OWN.at[0], OWN.at[0], target).wait_send())
    dual_out.wait()


def results(volume_in, dual_in, volume_out, dual_out, sems):
    copies = []
    for j in range(NZ):
        for k in range(4):
            copies.append(pltpu.make_async_copy(dual_in.at[0, k, j], dual_out.at[0, k, j], sems.at[k, j]))
        copies.append(pltpu.make_async_copy(volume_in.at[0, j], volume_out.at[0, j], sems.at[4, j]))
    for one in copies:
        one.start()
    for one in copies:
        one.wait()


def shards(volume, prior_image, dual_pairs, pair_cycle, pair_offset):
    image = pltpu.VMEM((NZ + 2, HALVES, ROWS, LANES), jnp.float32)
    block = pltpu.VMEM((NZ, HALVES, NY, LANES), jnp.float32)
    half = pltpu.VMEM((2, HALVES, NY, LANES), jnp.float32)
    plane = pltpu.VMEM((HALVES, ROWS, LANES), jnp.float32)
    stack = pltpu.VMEM((NZ + 2, HALVES, NY, LANES), jnp.float32)
    slots = pltpu.VMEM((4, NZ, HALVES, NY, LANES), jnp.float32)
    smem = pl.BlockSpec(memory_space=pltpu.SMEM)
    anyspace = pl.BlockSpec(memory_space=pl.ANY)
    volume_next, dual_next = pl.pallas_call(
        kernel,
        out_shape=(
            pltpu.VMEM(volume.shape, jnp.float32),
            pltpu.VMEM(dual_pairs.shape, jnp.float32),
        ),
        in_specs=[smem, smem, anyspace, anyspace, anyspace],
        out_specs=(pl.BlockSpec(memory_space=pltpu.VMEM), anyspace),
        scratch_shapes=[
            stack, image, image, image, image, plane, plane, block, block,
            stack, stack, stack, plane, plane, slots, slots,
            block, block, block, block, block, block,
            half, half, half, half, block, block,
            block, block, block,
            pltpu.SemaphoreType.DMA((len(NAMES),)),
            pltpu.SemaphoreType.DMA((len(NAMES),)),
            pltpu.SemaphoreType.DMA((7, HALVES)),
        ],
        compiler_params=pltpu.CompilerParams(collective_id=0, vmem_limit_bytes=61_790_000, has_side_effects=True),
    )(pair_cycle, pair_offset, volume, prior_image, dual_pairs)
    return pl.pallas_call(
        results,
        out_shape=(
            jax.ShapeDtypeStruct(volume.shape, jnp.float32),
            jax.ShapeDtypeStruct(dual_pairs.shape, jnp.float32),
        ),
        in_specs=[anyspace, anyspace],
        out_specs=(anyspace, anyspace),
        scratch_shapes=[pltpu.SemaphoreType.DMA((5, NZ))],
        compiler_params=pltpu.CompilerParams(vmem_limit_bytes=1024 * 1024),
    )(volume_next, dual_next)


def solution(mesh):
    return jax.shard_map(
        shards,
        mesh=mesh,
        in_specs=(
            P("tm", "space", None, None),
            P("tm", "space", None, None),
            P("tm", None, "space", None, None),
            P("tm", None),
            P("tm", None),
        ),
        out_specs=(P("tm", "space", None, None), P("tm", None, "space", None, None)),
        check_vma=False,
    )
```
